768 devices in a mesh: fsdp: 128 (over z_lo, x, y), dp: 6 (over z_hi, core).
Axes of the slice: x: 4, y: 8, z: 12 (z_hi: 3, z_lo: 4; z = z_hi * 4 + z_lo), core: 2. Of those that a mesh axis runs over, the one named last changes fastest.
Arguments:
- normed: bfloat16 [2, 98304, 4096], P(None, ('fsdp', 'dp')), may hold values from -6 to 6
- kv_cotangent: bfloat16 [2, 98304, 512], P(None, ('fsdp', 'dp')), may hold values from -6 to 6
- kv_weight: bfloat16 [4096, 512], P('fsdp'), may hold values from -0.09375 to 0.09375
- main_grad: float32 [4096, 512], P('fsdp'), may hold values from -6 to 6
- owner_order: int32 [128], replicated, may hold values from 0 to 127, each once
Outputs:
- key_rows: bfloat16 [2, 98304, 512], P(None, ('fsdp', 'dp'))
- input_grad: bfloat16 [2, 98304, 4096], P(None, ('fsdp', 'dp'))
- grad_buffer: float32 [4096, 512], P('fsdp')
The draws below stay inside these ranges and needn't reach their ends.
Inputs may be any that keep to these rules, and one draw needn't show every extreme that they name: `owner_order`: a permutation: each value appears once.
All inputs are finite; a program needn't handle non-finite values.
Results may differ from the reference program's by a relative error of at most 0.0075.
Values may be sent and summed in bfloat16 or wider, within the bound.
A program may use at most 64 MiB of HBM per device.

```python
import math
import jax
import jax.numpy as jnp
from jax import lax

D = 4096
MICRO = 2
TOK_DEV = 128
KVW = 512
TOKENS = 98304
N_FSDP = 128
N_DP = 6


def steps_of(rng, dims, split, smallest, high):
    level = 1.0
    for axis_at, blocks in split:
        heights = jax.random.uniform(jax.random.fold_in(jax.random.fold_in(rng, 6), axis_at), (blocks,), jnp.float32, smallest / len(split), high / len(split))
        level = level * jnp.repeat(jnp.exp(heights), dims[axis_at] // blocks).reshape((-1,) + (1,) * (len(dims) - 1 - axis_at))
    return level


def gaussian(rng, shape, scale, reach, cuts=(), kind=jnp.bfloat16):
    level = steps_of(rng, shape, cuts, -0.22, 0.18) if cuts else 1.0
    array = jax.random.normal(rng, shape, jnp.float32) * scale * level
    return jnp.minimum(jnp.maximum(array, -reach), reach).astype(kind)


def setup_inputs(seed: int = 0) -> dict:
    key_list = jax.random.split(jax.random.key(seed), 6)
    normed = gaussian(key_list[0], (MICRO, TOKENS, D), 1.0, 6.0, ((1, 768),))
    kv_cotangent = gaussian(key_list[1], (MICRO, TOKENS, KVW), 1.0, 6.0, ((1, 768),))
    kv_weight = gaussian(key_list[2], (D, KVW), D ** -0.5, 0.09375, ((0, 128),))
    main_grad = gaussian(key_list[3], (D, KVW), 1.0, 6.0, ((0, 128),), jnp.float32)
    owner_order = jax.random.permutation(key_list[4], N_FSDP).astype(jnp.int32)
    return dict(normed=normed, kv_cotangent=kv_cotangent, kv_weight=kv_weight, main_grad=main_grad, owner_order=owner_order)


def reference(normed, kv_cotangent, kv_weight, main_grad, owner_order):
    shard_rows = D // N_FSDP
    block_count = MICRO * N_DP
    block_rows = TOK_DEV * N_FSDP
    inverse_owner = jnp.argsort(owner_order).astype(jnp.int32)
    blocks_in = normed.reshape(block_count, block_rows, D)
    blocks_cot = kv_cotangent.reshape(block_count, block_rows, KVW)

    def advance(grad_sum, inputs_pair):
        inputs, cotangent = inputs_pair
        permuted = inputs.reshape(block_rows, N_FSDP, shard_rows)[:, owner_order, :].reshape(block_rows, D)
        key_block = jnp.dot(permuted, kv_weight, preferred_element_type=jnp.float32).astype(jnp.bfloat16)
        grad_permuted = jnp.dot(cotangent, kv_weight.T, preferred_element_type=jnp.float32).astype(jnp.bfloat16)
        grad_block = grad_permuted.reshape(block_rows, N_FSDP, shard_rows)[:, inverse_owner, :].reshape(block_rows, D)
        grad_sum = grad_sum + jnp.dot(permuted.T, cotangent, preferred_element_type=jnp.float32)
        return (grad_sum, (key_block, grad_block))
    grad_sum, outputs = lax.scan(advance, jnp.zeros((D, KVW), jnp.float32), (blocks_in, blocks_cot))
    key_blocks, grad_blocks = outputs
    grad_scale = 1.0 / math.sqrt(MICRO * TOKENS)
    grad_buffer = main_grad + grad_sum * grad_scale
    return (key_blocks.reshape(MICRO, TOKENS, KVW), grad_blocks.reshape(MICRO, TOKENS, D), grad_buffer)
```

```python
import functools
import math

import jax
import jax.numpy as jnp
from jax import lax
from jax.experimental import pallas as pl
from jax.experimental.pallas import tpu as pltpu
from jax.sharding import Mesh
from jax.sharding import PartitionSpec as P

MESH = pl.DeviceIdType.MESH
NAMES = ("zl", "x", "y", "zh", "core")
F32, BF16 = jnp.float32, jnp.bfloat16
CHUNK = 512
PLUS, MINUS = 0, 1


def kernel(
    ny, nh, scale,
    order, inv, normed, cot, weight, main, key_out, ig_out, gb_out,
    nv, cv, mv, grad, gw, ow, wv, igv, kacc, kv,
    snd, rcv, sq, tq, mq, r1, sp, tp, mp, r2, sy, yb, sh, hb, fb,
    loc, ays, ayr, aps, apr, aqs, aqr, ads, adr,
    rds, rdr, rqs, rqr, rps, rpr, rys, ryr, rhs, rhr, fin, out,
):
    half = ny // 2
    micro, tok, width = normed.shape
    rows, hw = gw.shape[1:]
    blocks_in_chunk = CHUNK // rows
    a, x, y = lax.axis_index("zl"), lax.axis_index("x"), lax.axis_index("y")
    h, c = lax.axis_index("zh"), lax.axis_index("core")
    nz = 4 * nh
    z = h * 4 + a

    def z_of(d):
        to = lax.rem(z + d + nz, nz)
        return lax.rem(to, 4), lax.div(to, 4)

    def heavy(d):
        az, hz = z_of(d)
        xx = lax.rem(x + d + 4, 4)
        return (a + (1 - c) * (az - a), x + c * (xx - x), y, h + (1 - c) * (hz - h), c)

    def light(d):
        az, hz = z_of(d)
        xx = lax.rem(x + d + 4, 4)
        return (a + c * (az - a), x + (1 - c) * (xx - x), y, h + c * (hz - h), c)

    q = a + c * (x - a)
    p = x + c * (a - x)
    partner = (a, x, y, h, 1 - c)
    heavies = (heavy(1), heavy(-1))
    lights = (light(1), light(-1))
    y_peers = [(a, x, lax.rem(y + d, ny), h, c) for d in range(1, ny)]
    h_peers = [(a, x, y, lax.rem(h + d, nh), c) for d in range(1, nh)]
    peers = [partner, *heavies, *lights, *y_peers, *h_peers]

    def rel(v, d):
        return lax.rem(v + d, 4)

    def slots(qq, pp):
        return (qq * 4 + pp) * ny

    def owner(cc, qq, pp):
        return ((qq + cc * (pp - qq)) * 4 + (pp + cc * (qq - pp))) * ny

    def remote(src, dst, s, r, to):
        return pltpu.make_async_remote_copy(
            src_ref=src, dst_ref=dst, send_sem=s, recv_sem=r, device_id=to, device_id_type=MESH
        )

    loads = [pltpu.make_async_copy(normed.at[m], nv.at[pl.ds(m * tok, tok)], loc.at[m]) for m in range(micro)]
    loads += [
        pltpu.make_async_copy(cot.at[m], cv.at[pl.ds(m * tok, tok)], loc.at[micro + m]) for m in range(micro)
    ]
    mine = slots(q, p) + y
    load_w = pltpu.make_async_copy(
        weight.at[:, pl.ds(pl.multiple_of(c * hw, hw), hw)], gw.at[mine], loc.at[2 * micro]
    )
    load_m = [
        pltpu.make_async_copy(main.at[:, pl.ds(k * hw, hw)], mv.at[k], loc.at[2 * micro + 1 + k]) for k in range(2)
    ]
    load_w.start()
    for copy in loads + load_m:
        copy.start()

    barrier = pltpu.get_barrier_semaphore()
    for peer in peers:
        pl.semaphore_signal(barrier, inc=1, device_id=peer, device_id_type=MESH)

    for copy in loads:
        copy.wait()

    def grad_chunk(i, carry):
        at = pl.multiple_of(i * CHUNK, CHUNK)
        d = lax.dot_general(
            nv[:, pl.ds(at, CHUNK)], cv[...], (((0,), (0,)), ((), ())), preferred_element_type=F32
        )
        first = i * blocks_in_chunk
        grad[0, pl.ds(first, blocks_in_chunk)] = d[:, :hw].reshape(blocks_in_chunk, rows, hw)
        grad[1, pl.ds(first, blocks_in_chunk)] = d[:, hw:].reshape(blocks_in_chunk, rows, hw)
        return carry

    lax.fori_loop(0, width // CHUNK, grad_chunk, 0)

    pl.semaphore_wait(barrier, len(peers))
    load_w.wait()
    ag_y = [
        remote(gw.at[mine], gw.at[mine], ays.at[d], ayr.at[d], y_peers[d]) for d in range(ny - 1)
    ]
    for copy in ag_y:
        copy.start()

    sent = list(ag_y)

    def send(copy):
        copy.start()
        sent.append(copy)
        return copy

    rs_d = {}
    for dq in (2, 1, 3, 0):
        for dp in (0, 1, 2, 3) if dq == 2 else (2, 1, 3, 0):
            qq, pp = rel(p, dq), rel(q, dp)
            st, base = slots(qq, pp), owner(1 - c, qq, pp)

            def convert(i, carry, st=st, base=base):
                snd[st + i] = grad[1 - c, order[base + i]].astype(BF16)
                return carry

            lax.fori_loop(0, ny, convert, 0, unroll=4)
            k = dq * 4 + dp
            rs_d[dq, dp] = send(
                remote(snd.at[pl.ds(st, ny)], rcv.at[pl.ds(st, ny)], rds.at[k], rdr.at[k], partner)
            )

    def summed(dq, dp, store, extra=()):
        qq, pp = rel(q, dq), rel(p, dp)
        st, base = slots(qq, pp), owner(c, qq, pp)

        def step(i, carry):
            v = grad[c, order[base + i]] + rcv[st + i].astype(F32)
            for ref in extra:
                v += ref[i].astype(F32)
            store(st, i, v)
            return carry

        lax.fori_loop(0, ny, step, 0, unroll=4)
        return st

    def to_sq(st, i, v):
        sq[st + i] = v.astype(BF16)

    two_away = {PLUS: (0, 2), MINUS: (1, 3)}

    rs_t = {}
    for k in range(2):
        for way in (PLUS, MINUS):
            dp = two_away[way][k]
            rs_d[2, dp].wait_recv()
            st = summed(2, dp, to_sq)
            rs_t[way, k] = send(
                remote(sq.at[pl.ds(st, ny)], tq.at[way, k], rqs.at[way, 4 + k], rqr.at[way, 4 + k], heavies[way])
            )

    rs_m = {}

    def rs_main(way, dp, extra=()):
        dq = 1 if way == PLUS else 3
        rs_d[dq, dp].wait_recv()
        st = summed(dq, dp, to_sq, extra)
        rs_m[way, dp] = send(
            remote(sq.at[pl.ds(st, ny)], mq.at[way, dp], rqs.at[way, dp], rqr.at[way, dp], heavies[way])
        )

    rs_main(MINUS, 2)
    rs_main(PLUS, 1)
    rs_main(PLUS, 3)
    rs_main(MINUS, 0)

    for copy in ag_y:
        copy.wait_recv()
    ag_p, ag_q, ag_d = {}, {}, {}

    def piece(dq, dp):
        return gw.at[pl.ds(slots(rel(q, dq), rel(p, dp)), ny)]

    def half_piece(dq, dp, j):
        return gw.at[pl.ds(slots(rel(q, dq), rel(p, dp)) + j * half, half)]

    def ag_light(way, dp, j, k):
        ag_p[way, k] = send(
            remote(half_piece(0, dp, j), half_piece(0, dp, j), aps.at[way, k], apr.at[way, k], lights[way])
        )

    def ag_heavy(way, dq, dp, k):
        ag_q[way, k] = send(remote(piece(dq, dp), piece(dq, dp), aqs.at[way, k], aqr.at[way, k], heavies[way]))

    def ag_across(dq, dp):
        st = slots(rel(q, dq), rel(p, dp))
        k = dq * 4 + dp
        ag_d[k] = send(remote(gw.at[pl.ds(st, ny)], ow.at[pl.ds(st, ny)], ads.at[k], adr.at[k], partner))

    ag_light(PLUS, 0, 0, 0)
    ag_light(MINUS, 0, 1, 1)
    ag_light(PLUS, 0, 1, 1)
    ag_light(MINUS, 0, 0, 0)

    for k in (1, 0):
        rs_t[PLUS, k].wait_recv()
        rs_main(PLUS, two_away[PLUS][k], (tq.at[PLUS, k],))
        rs_t[MINUS, k].wait_recv()
        rs_main(MINUS, two_away[MINUS][k], (tq.at[MINUS, k],))

    def ag_own(dp):
        ag_heavy(PLUS, 0, dp, dp)
        ag_heavy(MINUS, 0, dp, dp)
        ag_across(0, dp)

    ag_own(0)
    ag_p[PLUS, 0].wait_recv()
    ag_light(PLUS, 3, 0, 2)
    ag_p[MINUS, 1].wait_recv()
    ag_light(MINUS, 1, 1, 2)
    ag_p[PLUS, 1].wait_recv()
    ag_own(3)
    ag_p[MINUS, 0].wait_recv()
    ag_own(1)
    ag_p[PLUS, 2].wait_recv()
    ag_p[MINUS, 2].wait_recv()
    ag_own(2)

    def heavy_sum(dp):
        rs_d[0, dp].wait_recv()
        rs_m[PLUS, dp].wait_recv()
        rs_m[MINUS, dp].wait_recv()

        def store(st, i, v):
            r1[dp, i] = v

        summed(0, dp, store, (mq.at[PLUS, dp], mq.at[MINUS, dp]))

    rs_pt, rs_pm = {}, {}

    def light_send(way, dp, j, dst, k, table, extra=None):
        def step(i, carry):
            v = r1[dp, j * half + i]
            if extra is not None:
                v += extra[i].astype(F32)
            sp[dp, j * half + i] = v.astype(BF16)
            return carry

        lax.fori_loop(0, half, step, 0, unroll=True)
        table[way, j] = send(
            remote(sp.at[dp, pl.ds(j * half, half)], dst, rps.at[way, k], rpr.at[way, k], lights[way])
        )

    heavy_sum(2)
    light_send(PLUS, 2, 0, tp.at[PLUS], 2, rs_pt)
    light_send(MINUS, 2, 1, tp.at[MINUS], 2, rs_pt)
    heavy_sum(1)
    light_send(PLUS, 1, 1, mp.at[PLUS, pl.ds(half, half)], 1, rs_pm)
    heavy_sum(3)
    light_send(MINUS, 3, 0, mp.at[MINUS, pl.ds(0, half)], 0, rs_pm)
    heavy_sum(0)

    forwards = {PLUS: (0, 1), MINUS: (3, 2)}

    def ag_arrived(way, dp):
        ag_q[way, dp].wait_recv()
        dq = 3 if way == PLUS else 1
        if dp in forwards[way]:
            ag_heavy(way, dq, dp, 4 + forwards[way].index(dp))
        ag_across(dq, dp)

    ag_arrived(PLUS, 0)
    ag_arrived(MINUS, 0)
    ag_arrived(PLUS, 3)
    ag_arrived(MINUS, 3)

    rs_pt[PLUS, 0].wait_recv()
    light_send(PLUS, 1, 0, mp.at[PLUS, pl.ds(0, half)], 0, rs_pm, tp.at[PLUS])
    rs_pt[MINUS, 1].wait_recv()
    light_send(MINUS, 3, 1, mp.at[MINUS, pl.ds(half, half)], 1, rs_pm, tp.at[MINUS])

    ag_arrived(PLUS, 1)
    ag_arrived(MINUS, 1)
    ag_arrived(PLUS, 2)
    ag_arrived(MINUS, 2)

    for copy in rs_pm.values():
        copy.wait_recv()

    def light_sum(i, carry):
        v = r1[0, i] + mp[PLUS, i].astype(F32) + mp[MINUS, i].astype(F32)
        r2[i] = v
        sy[i] = v.astype(BF16)
        return carry

    lax.fori_loop(0, ny, light_sum, 0, unroll=4)
    rs_y = [
        send(remote(sy.at[lax.rem(y + d + 1, ny)], yb.at[d], rys.at[d], ryr.at[d], y_peers[d]))
        for d in range(ny - 1)
    ]

    for way in (PLUS, MINUS):
        for k in range(2):
            ag_q[way, 4 + k].wait_recv()
            ag_across(2, forwards[way][k])

    for copy in rs_y:
        copy.wait_recv()
    total = r2[y]
    for d in range(ny - 1):
        total += yb[d].astype(F32)
    rounded = total.astype(BF16)
    sh[...] = rounded
    hb[h] = rounded
    rs_h = [send(remote(sh, hb.at[h], rhs.at[d], rhr.at[d], h_peers[d])) for d in range(nh - 1)]

    for copy in ag_d.values():
        copy.wait_recv()

    def place(o, carry):
        f = inv[o]
        swapped = lax.rem(f, ny) + (lax.rem(lax.div(f, ny), 4) * 4 + lax.div(f, 4 * ny)) * ny
        at = pl.ds(pl.multiple_of(o * rows, rows), rows)
        wv[c, at] = gw[f + c * (swapped - f)]
        wv[1 - c, at] = ow[f + (1 - c) * (swapped - f)]
        return carry

    lax.fori_loop(0, gw.shape[0], place, 0, unroll=4)

    kacc[...] = jnp.zeros_like(kacc)

    def product(i, carry):
        at = pl.ds(pl.multiple_of(i * CHUNK, CHUNK), CHUNK)
        w0, w1 = wv[0, at], wv[1, at]
        n = nv[:, at]
        kacc[0] += jnp.dot(n, w0, preferred_element_type=F32)
        kacc[1] += jnp.dot(n, w1, preferred_element_type=F32)
        contract = (((1,), (1,)), ((), ()))
        g = lax.dot_general(cv[:, :hw], w0, contract, preferred_element_type=F32)
        g += lax.dot_general(cv[:, hw:], w1, contract, preferred_element_type=F32)
        igv[:, at] = g.astype(BF16)
        return carry

    lax.fori_loop(0, width // CHUNK, product, 0)
    kv[:, :hw] = kacc[0].astype(BF16)
    kv[:, hw:] = kacc[1].astype(BF16)
    stores = [pltpu.make_async_copy(igv.at[pl.ds(m * tok, tok)], ig_out.at[m], out.at[m]) for m in range(micro)]
    stores += [
        pltpu.make_async_copy(kv.at[pl.ds(m * tok, tok)], key_out.at[m], out.at[micro + m]) for m in range(micro)
    ]
    for copy in stores:
        copy.start()

    for copy in rs_h:
        copy.wait_recv()
    for copy in load_m:
        copy.wait()
    total = hb[0].astype(F32)
    for k in range(1, nh):
        total += hb[k].astype(F32)
    fb[c] = mv[c] + total * scale
    last = send(remote(fb.at[c], fb.at[c], fin.at[0], fin.at[1], partner))
    last.wait_recv()
    for k in range(2):
        stores.append(pltpu.make_async_copy(fb.at[k], gb_out.at[:, pl.ds(k * hw, hw)], out.at[2 * micro + k]))
        stores[-1].start()
    for copy in sent:
        copy.wait_send()
    for copy in stores:
        copy.wait()


def body(ny, nh, normed, kv_cotangent, kv_weight, main_grad, owner_order):
    micro, tok, width = normed.shape
    rows, key_width = kv_weight.shape
    owners = 16 * ny
    hw = key_width // 2
    half = ny // 2
    everyone = owners * nh * 2
    scale = 1.0 / math.sqrt(micro * tok * everyone)
    indices = jnp.arange(owners, dtype=jnp.int32)
    inv = jnp.sum(jnp.where(owner_order[None, :] == indices[:, None], indices[None, :], 0), axis=1)
    dma = pltpu.SemaphoreType.DMA
    anywhere = pl.BlockSpec(memory_space=pl.ANY)
    scalars = pl.BlockSpec(memory_space=pltpu.SMEM)
    block = (rows, hw)
    return pl.pallas_call(
        functools.partial(kernel, ny, nh, scale),
        out_shape=(
            jax.ShapeDtypeStruct((micro, tok, key_width), BF16),
            jax.ShapeDtypeStruct((micro, tok, width), BF16),
            jax.ShapeDtypeStruct((rows, key_width), F32),
        ),
        in_specs=[scalars, scalars] + [anywhere] * 4,
        out_specs=(anywhere,) * 3,
        scratch_shapes=[
            pltpu.VMEM((micro * tok, width), BF16),
            pltpu.VMEM((micro * tok, key_width), BF16),
            pltpu.VMEM((2, *block), F32),
            pltpu.VMEM((2, owners, *block), F32),
            pltpu.VMEM((owners, *block), BF16),
            pltpu.VMEM((owners, *block), BF16),
            pltpu.VMEM((2, width, hw), BF16),
            pltpu.VMEM((micro * tok, width), BF16),
            pltpu.VMEM((2, micro * tok, hw), F32),
            pltpu.VMEM((micro * tok, key_width), BF16),
            pltpu.VMEM((owners, *block), BF16),
            pltpu.VMEM((owners, *block), BF16),
            pltpu.VMEM((owners, *block), BF16),
            pltpu.VMEM((2, 2, ny, *block), BF16),
            pltpu.VMEM((2, 4, ny, *block), BF16),
            pltpu.VMEM((4, ny, *block), F32),
            pltpu.VMEM((4, ny, *block), BF16),
            pltpu.VMEM((2, half, *block), BF16),
            pltpu.VMEM((2, ny, *block), BF16),
            pltpu.VMEM((ny, *block), F32),
            pltpu.VMEM((ny, *block), BF16),
            pltpu.VMEM((ny - 1, *block), BF16),
            pltpu.VMEM(block, BF16),
            pltpu.VMEM((nh, *block), BF16),
            pltpu.VMEM((2, *block), F32),
            dma((2 * micro + 3,)),
            dma((ny - 1,)),
            dma((ny - 1,)),
            dma((2, 3)),
            dma((2, 3)),
            dma((2, 6)),
            dma((2, 6)),
            dma((16,)),
            dma((16,)),
            dma((16,)),
            dma((16,)),
            dma((2, 6)),
            dma((2, 6)),
            dma((2, 3)),
            dma((2, 3)),
            dma((ny - 1,)),
            dma((ny - 1,)),
            dma((max(nh - 1, 1),)),
            dma((max(nh - 1, 1),)),
            dma((2,)),
            dma((2 * micro + 2,)),
        ],
        compiler_params=pltpu.CompilerParams(
            collective_id=0, has_side_effects=True, vmem_limit_bytes=60 * 1024 * 1024
        ),
    )(owner_order, inv, normed, kv_cotangent, kv_weight, main_grad)


def solution(mesh):
    owners = mesh.shape["fsdp"]
    ny, nh = owners // 16, mesh.shape["dp"] // 2
    split = Mesh(mesh.devices.reshape(4, 4, ny, nh, 2), NAMES)
    tokens, fsdp = P(None, NAMES, None), P(NAMES[:3], None)
    return jax.shard_map(
        functools.partial(body, ny, nh),
        mesh=split,
        in_specs=(tokens, tokens, fsdp, fsdp, P()),
        out_specs=(tokens, tokens, fsdp),
        check_vma=False,
    )
```

```python
import functools
import math

import jax
import jax.numpy as jnp
from jax import lax
from jax.experimental import pallas as pl
from jax.experimental.pallas import tpu as pltpu
from jax.sharding import Mesh
from jax.sharding import PartitionSpec as P

MESH = pl.DeviceIdType.MESH
NAMES = ("zl", "x", "y", "zh", "core")
F32, BF16 = jnp.float32, jnp.bfloat16
CHUNK = 512
PLUS, MINUS = 0, 1


def kernel(
    ny, nh, scale,
    order_in, normed, cot, weight, main, key_out, ig_out, gb_out,
    order, inv, inv_row, nv, cv, mv, grad, gow, kacc,
    snd, rcv, sq, tq, mq, r1, sp, tp, mp, r2, sy, yb, sh, hb, fb,
    loc, out, ayr, apr, aqr, adr, rdr, rqr, rpr, ryr, rhr, fin,
):
    half = ny // 2
    micro, tok, width = normed.shape
    owners, rows, hw = gow.shape[1:]
    blocks_in_chunk = CHUNK // rows
    a, x, y = lax.axis_index("zl"), lax.axis_index("x"), lax.axis_index("y")
    h, c = lax.axis_index("zh"), lax.axis_index("core")
    nz = 4 * nh
    gw, ow = gow.at[c], gow.at[1 - c]
    z = h * 4 + a

    def z_of(d):
        to = lax.rem(z + d + nz, nz)
        return lax.rem(to, 4), lax.div(to, 4)

    def heavy(d):
        az, hz = z_of(d)
        xx = lax.rem(x + d + 4, 4)
        return (a + (1 - c) * (az - a), x + c * (xx - x), y, h + (1 - c) * (hz - h), c)

    def light(d):
        az, hz = z_of(d)
        xx = lax.rem(x + d + 4, 4)
        return (a + c * (az - a), x + (1 - c) * (xx - x), y, h + c * (hz - h), c)

    q = a + c * (x - a)
    p = x + c * (a - x)
    partner = (a, x, y, h, 1 - c)
    heavies = (heavy(1), heavy(-1))
    lights = (light(1), light(-1))
    y_peers = [(a, x, lax.rem(y + d, ny), h, c) for d in range(1, ny)]
    h_peers = [(a, x, y, lax.rem(h + d, nh), c) for d in range(1, nh)]
    peers = [partner, *heavies, *lights, *y_peers, *h_peers]

    def rel(v, d):
        return lax.rem(v + d, 4)

    def slots(qq, pp):
        return (qq * 4 + pp) * ny

    def owner(cc, qq, pp):
        return ((qq + cc * (pp - qq)) * 4 + (pp + cc * (qq - pp))) * ny

    def remote(src, dst, s, r, to):
        return pltpu.make_async_remote_copy(
            src_ref=src, dst_ref=dst, send_sem=s, recv_sem=r, device_id=to, device_id_type=MESH
        )

    mine = slots(q, p) + y
    load_w = pltpu.make_async_copy(
        weight.at[:, pl.ds(pl.multiple_of(c * hw, hw), hw)], gow.at[c, mine], loc.at[0]
    )
    load_order = pltpu.make_async_copy(order_in, order, loc.at[1])
    loads = [
        pltpu.make_async_copy(cot.at[m], cv.at[pl.ds(m * tok, tok)], loc.at[2 + m]) for m in range(micro)
    ]
    wide = width // 2
    loads_n = [
        [
            pltpu.make_async_copy(
                normed.at[m, :, pl.ds(k * wide, wide)],
                nv.at[pl.ds(m * tok, tok), pl.ds(k * wide, wide)],
                loc.at[2 + (k + 1) * micro + m],
            )
            for m in range(micro)
        ]
        for k in range(2)
    ]
    load_m = [
        pltpu.make_async_copy(main.at[:, pl.ds(k * hw, hw)], mv.at[k], loc.at[2 + 3 * micro + k]) for k in range(2)
    ]
    load_w.start()
    for copy in loads + loads_n[0] + loads_n[1] + [load_order] + load_m:
        copy.start()

    barrier = pltpu.get_barrier_semaphore()
    for peer in peers:
        pl.semaphore_signal(barrier, inc=1, device_id=peer, device_id_type=MESH)

    def grad_chunk(i, carry):
        at = pl.multiple_of(i * CHUNK, CHUNK)
        d = lax.dot_general(
            nv[:, pl.ds(at, CHUNK)], cv[...], (((0,), (0,)), ((), ())), preferred_element_type=F32
        )
        first = i * blocks_in_chunk
        grad[0, pl.ds(first, blocks_in_chunk)] = d[:, :hw].reshape(blocks_in_chunk, rows, hw)
        grad[1, pl.ds(first, blocks_in_chunk)] = d[:, hw:].reshape(blocks_in_chunk, rows, hw)
        return carry

    chunks = width // CHUNK
    sent = []

    def send(copy, group, size):
        copy.start()
        sent.append((group, size))
        return copy

    for copy in loads + loads_n[0]:
        copy.wait()
    lax.fori_loop(0, chunks // 2, grad_chunk, 0)
    load_w.wait()
    pl.semaphore_wait(barrier, len(peers))
    ag_y = [
        send(remote(gow.at[c, mine], gow.at[c, mine], out.at[0], ayr.at[0], y_peers[d]), 0, 1)
        for d in range(ny - 1)
    ]
    for copy in loads_n[1]:
        copy.wait()
    lax.fori_loop(chunks // 2, chunks, grad_chunk, 0)
    load_order.wait()

    rs_d = {}
    for dq in (2, 1, 3, 0):
        for dp in (0, 1, 2, 3) if dq == 2 else (2, 1, 3, 0):
            qq, pp = rel(p, dq), rel(q, dp)
            st, base = slots(qq, pp), owner(1 - c, qq, pp)

            def convert(i, carry, st=st, base=base):
                snd[st + i] = grad[1 - c, order[0, base + i]].astype(BF16)
                return carry

            lax.fori_loop(0, ny, convert, 0, unroll=4)
            rs_d[dq, dp] = send(
                remote(snd.at[pl.ds(st, ny)], rcv.at[pl.ds(st, ny)], out.at[1], rdr.at[dq * 4 + dp], partner), 1, ny
            )

    def summed(dq, dp, store, extra=()):
        qq, pp = rel(q, dq), rel(p, dp)
        st, base = slots(qq, pp), owner(c, qq, pp)

        def step(i, carry):
            v = grad[c, order[0, base + i]] + rcv[st + i].astype(F32)
            for ref in extra:
                v += ref[i].astype(F32)
            store(st, i, v)
            return carry

        lax.fori_loop(0, ny, step, 0, unroll=4)
        return st

    def to_sq(st, i, v):
        sq[st + i] = v.astype(BF16)

    two_away = {PLUS: (0, 2), MINUS: (1, 3)}

    rs_t = {}
    for k in range(2):
        for way in (PLUS, MINUS):
            dp = two_away[way][k]
            rs_d[2, dp].wait_recv()
            st = summed(2, dp, to_sq)
            rs_t[way, k] = send(
                remote(sq.at[pl.ds(st, ny)], tq.at[way, k], out.at[2], rqr.at[way, 4 + k], heavies[way]), 2, ny
            )

    rs_m = {}

    def rs_main(way, dp, extra=()):
        dq = 1 if way == PLUS else 3
        rs_d[dq, dp].wait_recv()
        st = summed(dq, dp, to_sq, extra)
        rs_m[way, dp] = send(
            remote(sq.at[pl.ds(st, ny)], mq.at[way, dp], out.at[2], rqr.at[way, dp], heavies[way]), 2, ny
        )

    rs_main(MINUS, 2)
    rs_main(PLUS, 1)
    rs_main(PLUS, 3)
    rs_main(MINUS, 0)

    lane = lax.broadcasted_iota(jnp.int32, (1, owners), 1)

    def invert(f, row):
        return jnp.where(lane == order[0, f], f, row)

    inv_row[...] = lax.fori_loop(0, owners, invert, jnp.zeros((1, owners), jnp.int32), unroll=8)
    load_inv = pltpu.make_async_copy(inv_row, inv, loc.at[0])
    load_inv.start()

    def total(ref, n):
        return ref.at[pl.ds(0, n)]

    def wait_all(ref, n, sem, to):
        remote(total(ref, n), total(ref, n), out.at[0], sem, to).wait_recv()

    wait_all(snd, ny - 1, ayr.at[0], partner)
    ag_p, ag_q = {}, {}

    def piece(dq, dp):
        return gow.at[c, pl.ds(slots(rel(q, dq), rel(p, dp)), ny)]

    def half_piece(dq, dp, j):
        return gow.at[c, pl.ds(slots(rel(q, dq), rel(p, dp)) + j * half, half)]

    def ag_light(way, dp, j, k):
        ag_p[way, k] = send(
            remote(half_piece(0, dp, j), half_piece(0, dp, j), out.at[3], apr.at[way, k], lights[way]), 3, half
        )

    def ag_heavy(way, dq, dp, k):
        ag_q[way, k] = send(
            remote(piece(dq, dp), piece(dq, dp), out.at[4], aqr.at[way, k], heavies[way]), 4, ny
        )

    def ag_across(dq, dp):
        send(remote(piece(dq, dp), piece(dq, dp), out.at[5], adr.at[0], partner), 5, ny)

    ag_light(PLUS, 0, 0, 0)
    ag_light(MINUS, 0, 1, 1)
    ag_light(PLUS, 0, 1, 1)
    ag_light(MINUS, 0, 0, 0)

    for k in (1, 0):
        rs_t[PLUS, k].wait_recv()
        rs_main(PLUS, two_away[PLUS][k], (tq.at[PLUS, k],))
        rs_t[MINUS, k].wait_recv()
        rs_main(MINUS, two_away[MINUS][k], (tq.at[MINUS, k],))

    def ag_own(dp):
        ag_heavy(PLUS, 0, dp, dp)
        ag_heavy(MINUS, 0, dp, dp)
        ag_across(0, dp)

    ag_own(0)
    ag_p[PLUS, 0].wait_recv()
    ag_light(PLUS, 3, 0, 2)
    ag_p[MINUS, 1].wait_recv()
    ag_light(MINUS, 1, 1, 2)
    ag_p[PLUS, 1].wait_recv()
    ag_own(3)
    ag_p[MINUS, 0].wait_recv()
    ag_own(1)
    ag_p[PLUS, 2].wait_recv()
    ag_p[MINUS, 2].wait_recv()
    ag_own(2)

    def heavy_sum(dp):
        rs_d[0, dp].wait_recv()
        rs_m[PLUS, dp].wait_recv()
        rs_m[MINUS, dp].wait_recv()

        def store(st, i, v):
            r1[dp, i] = v

        summed(0, dp, store, (mq.at[PLUS, dp], mq.at[MINUS, dp]))

    rs_pt, rs_pm = {}, {}

    def light_send(way, dp, j, dst, k, table, extra=None):
        def step(i, carry):
            v = r1[dp, j * half + i]
            if extra is not None:
                v += extra[i].astype(F32)
            sp[dp, j * half + i] = v.astype(BF16)
            return carry

        lax.fori_loop(0, half, step, 0, unroll=True)
        table[way, j] = send(
            remote(sp.at[dp, pl.ds(j * half, half)], dst, out.at[6], rpr.at[way, k], lights[way]), 6, half
        )

    heavy_sum(2)
    light_send(PLUS, 2, 0, tp.at[PLUS], 2, rs_pt)
    light_send(MINUS, 2, 1, tp.at[MINUS], 2, rs_pt)
    heavy_sum(1)
    light_send(PLUS, 1, 1, mp.at[PLUS, pl.ds(half, half)], 1, rs_pm)
    heavy_sum(3)
    light_send(MINUS, 3, 0, mp.at[MINUS, pl.ds(0, half)], 0, rs_pm)
    heavy_sum(0)

    forwards = {PLUS: (0, 1), MINUS: (3, 2)}

    def ag_arrived(way, dp):
        ag_q[way, dp].wait_recv()
        dq = 3 if way == PLUS else 1
        if dp in forwards[way]:
            ag_heavy(way, dq, dp, 4 + forwards[way].index(dp))
        ag_across(dq, dp)

    ag_arrived(PLUS, 0)
    ag_arrived(MINUS, 0)
    ag_arrived(PLUS, 3)
    ag_arrived(MINUS, 3)

    rs_pt[PLUS, 0].wait_recv()
    light_send(PLUS, 1, 0, mp.at[PLUS, pl.ds(0, half)], 0, rs_pm, tp.at[PLUS])
    rs_pt[MINUS, 1].wait_recv()
    light_send(MINUS, 3, 1, mp.at[MINUS, pl.ds(half, half)], 1, rs_pm, tp.at[MINUS])

    ag_arrived(PLUS, 1)
    ag_arrived(MINUS, 1)
    ag_arrived(PLUS, 2)
    ag_arrived(MINUS, 2)

    for copy in rs_pm.values():
        copy.wait_recv()

    def light_sum(i, carry):
        v = r1[0, i] + mp[PLUS, i].astype(F32) + mp[MINUS, i].astype(F32)
        r2[i] = v
        sy[i] = v.astype(BF16)
        return carry

    lax.fori_loop(0, ny, light_sum, 0, unroll=4)
    rs_y = [
        send(remote(sy.at[lax.rem(y + d + 1, ny)], yb.at[d], out.at[7], ryr.at[0], y_peers[d]), 7, 1)
        for d in range(ny - 1)
    ]

    for way in (PLUS, MINUS):
        for k in range(2):
            ag_q[way, 4 + k].wait_recv()
            ag_across(2, forwards[way][k])

    wait_all(yb, ny - 1, ryr.at[0], partner)
    value = r2[y]
    for d in range(ny - 1):
        value += yb[d].astype(F32)
    rounded = value.astype(BF16)
    sh[...] = rounded
    hb[h] = rounded
    rs_h = [send(remote(sh, hb.at[h], out.at[8], rhr.at[0], h_peers[d]), 8, 1) for d in range(nh - 1)]

    load_inv.wait()
    remote(gow.at[c], gow.at[1 - c], out.at[0], adr.at[0], partner).wait_recv()

    kacc[...] = jnp.zeros_like(kacc)
    contract = (((1,), (1,)), ((), ()))

    def product(i, carry):
        at = pl.ds(pl.multiple_of(i * CHUNK, CHUNK), CHUNK)
        fs = [inv[0, i * blocks_in_chunk + b] for b in range(blocks_in_chunk)]
        swapped = [lax.rem(f, ny) + (lax.rem(lax.div(f, ny), 4) * 4 + lax.div(f, 4 * ny)) * ny for f in fs]
        w0 = jnp.concatenate([gow[0, f] for f in fs], axis=0)
        w1 = jnp.concatenate([gow[1, f] for f in swapped], axis=0)
        n = nv[:, at]
        kacc[0] += jnp.dot(n, w0, preferred_element_type=F32)
        kacc[1] += jnp.dot(n, w1, preferred_element_type=F32)
        g = lax.dot_general(cv[:, :hw], w0, contract, preferred_element_type=F32)
        g += lax.dot_general(cv[:, hw:], w1, contract, preferred_element_type=F32)
        ig_out[:, at] = g.astype(BF16)
        return carry

    lax.fori_loop(0, chunks, product, 0)
    key_out[:, :hw] = kacc[0].astype(BF16)
    key_out[:, hw:] = kacc[1].astype(BF16)

    if nh > 1:
        wait_all(hb, nh - 1, rhr.at[0], partner)
    for copy in load_m:
        copy.wait()
    value = hb[0].astype(F32)
    for k in range(1, nh):
        value += hb[k].astype(F32)
    fb[c] = mv[c] + value * scale
    last = send(remote(fb.at[c], fb.at[c], out.at[9], fin.at[0], partner), 9, 1)
    last.wait_recv()
    gb_out[:, :hw] = fb[0]
    gb_out[:, hw:] = fb[1]
    sizes = {}
    for group, size in sent:
        sizes[group] = sizes.get(group, 0) + size
    for group, size in sizes.items():
        ref = total(fb if group == 9 else snd, size)
        remote(ref, ref, out.at[group], fin.at[0], partner).wait_send()


def store(ig, key, gb, ig_out, key_out, gb_out, sems):
    micro, tok, width = ig_out.shape
    copies = [pltpu.make_async_copy(gb, gb_out, sems.at[2 * micro])]
    for m in range(micro):
        copies.append(pltpu.make_async_copy(ig.at[pl.ds(m * tok, tok)], ig_out.at[m], sems.at[m]))
        copies.append(pltpu.make_async_copy(key.at[pl.ds(m * tok, tok)], key_out.at[m], sems.at[micro + m]))
    for copy in copies:
        copy.start()
    for copy in copies:
        copy.wait()


def body(ny, nh, normed, kv_cotangent, kv_weight, main_grad, owner_order):
    micro, tok, width = normed.shape
    rows, key_width = kv_weight.shape
    owners = 16 * ny
    hw = key_width // 2
    half = ny // 2
    everyone = owners * nh * 2
    scale = 1.0 / math.sqrt(micro * tok * everyone)
    dma = pltpu.SemaphoreType.DMA
    anywhere = pl.BlockSpec(memory_space=pl.ANY)
    vmem = pl.BlockSpec(memory_space=pltpu.VMEM)
    block = (rows, hw)
    all_rows = micro * tok
    key, ig, gb = pl.pallas_call(
        functools.partial(kernel, ny, nh, scale),
        out_shape=(
            pltpu.VMEM((all_rows, key_width), BF16),
            pltpu.VMEM((all_rows, width), BF16),
            pltpu.VMEM((rows, key_width), F32),
        ),
        in_specs=[anywhere] * 5,
        out_specs=(vmem,) * 3,
        scratch_shapes=[
            pltpu.SMEM((1, owners), jnp.int32),
            pltpu.SMEM((1, owners), jnp.int32),
            pltpu.VMEM((1, owners), jnp.int32),
            pltpu.VMEM((all_rows, width), BF16),
            pltpu.VMEM((all_rows, key_width), BF16),
            pltpu.VMEM((2, *block), F32),
            pltpu.VMEM((2, owners, *block), F32),
            pltpu.VMEM((2, owners, *block), BF16),
            pltpu.VMEM((2, all_rows, hw), F32),
            pltpu.VMEM((owners, *block), BF16),
            pltpu.VMEM((owners, *block), BF16),
            pltpu.VMEM((owners, *block), BF16),
            pltpu.VMEM((2, 2, ny, *block), BF16),
            pltpu.VMEM((2, 4, ny, *block), BF16),
            pltpu.VMEM((4, ny, *block), F32),
            pltpu.VMEM((4, ny, *block), BF16),
            pltpu.VMEM((2, half, *block), BF16),
            pltpu.VMEM((2, ny, *block), BF16),
            pltpu.VMEM((ny, *block), F32),
            pltpu.VMEM((ny, *block), BF16),
            pltpu.VMEM((ny - 1, *block), BF16),
            pltpu.VMEM(block, BF16),
            pltpu.VMEM((nh, *block), BF16),
            pltpu.VMEM((2, *block), F32),
            dma((3 * micro + 4,)),
            dma((10,)),
            dma((1,)),
            dma((2, 3)),
            dma((2, 6)),
            dma((1,)),
            dma((16,)),
            dma((2, 6)),
            dma((2, 3)),
            dma((1,)),
            dma((1,)),
            dma((1,)),
        ],
        compiler_params=pltpu.CompilerParams(
            collective_id=0, has_side_effects=True, vmem_limit_bytes=56 * 1024 * 1024
        ),
    )(owner_order.reshape(1, owners), normed, kv_cotangent, kv_weight, main_grad)
    ig, key, gb = pl.pallas_call(
        store,
        out_shape=(
            jax.ShapeDtypeStruct((micro, tok, width), BF16),
            jax.ShapeDtypeStruct((micro, tok, key_width), BF16),
            jax.ShapeDtypeStruct((rows, key_width), F32),
        ),
        in_specs=[anywhere] * 3,
        out_specs=(anywhere,) * 3,
        scratch_shapes=[dma((2 * micro + 1,))],
        compiler_params=pltpu.CompilerParams(vmem_limit_bytes=1024 * 1024),
    )(ig, key, gb)
    return key, ig, gb


def solution(mesh):
    owners = mesh.shape["fsdp"]
    ny, nh = owners // 16, mesh.shape["dp"] // 2
    split = Mesh(mesh.devices.reshape(4, 4, ny, nh, 2), NAMES)
    tokens, fsdp = P(None, NAMES, None), P(NAMES[:3], None)
    return jax.shard_map(
        functools.partial(body, ny, nh),
        mesh=split,
        in_specs=(tokens, tokens, fsdp, fsdp, P()),
        out_specs=(tokens, tokens, fsdp),
        check_vma=False,
    )
```

```python
import functools
import math

import jax
import jax.numpy as jnp
from jax import lax
from jax.experimental import pallas as pl
from jax.experimental.pallas import tpu as pltpu
from jax.sharding import Mesh
from jax.sharding import PartitionSpec as P

MESH = pl.DeviceIdType.MESH
NAMES = ("zl", "x", "y", "zh", "core")
F32, BF16 = jnp.float32, jnp.bfloat16
CHUNK = 512
PLUS, MINUS = 0, 1
UNITS = ((3, 4), (5, 6), (2, 1), (7, 0))


def kernel(
    ny, nh, scale,
    order_in, normed, cot, weight, main, key_out, ig_out, gb_out,
    order, inv, inv_row, nv, cv, mv, turned, gow, kacc,
    snd, rcv, sq, tq, mq, sy, ty, hy, my, r2, pb, sh, hb, fb,
    loc, out, apr, ayr, aqr, adr, rdr, rqr, ryr, rpr, rhr, fin,
):
    micro, tok, width = normed.shape
    owners, rows, hw = gow.shape[1:]
    blocks_in_chunk = CHUNK // rows
    a, x, y = lax.axis_index("zl"), lax.axis_index("x"), lax.axis_index("y")
    h, c = lax.axis_index("zh"), lax.axis_index("core")
    nz = 4 * nh
    z = h * 4 + a

    def z_of(d):
        to = lax.rem(z + d + nz, nz)
        return lax.rem(to, 4), lax.div(to, 4)

    def heavy(d):
        az, hz = z_of(d)
        xx = lax.rem(x + d + 4, 4)
        return (a + (1 - c) * (az - a), x + c * (xx - x), y, h + (1 - c) * (hz - h), c)

    def light(d):
        az, hz = z_of(d)
        xx = lax.rem(x + d + 4, 4)
        return (a + c * (az - a), x + (1 - c) * (xx - x), y, h + c * (hz - h), c)

    def along(d):
        return (a, x, lax.rem(y + d + ny, ny), h, c)

    q = a + c * (x - a)
    p = x + c * (a - x)
    partner = (a, x, y, h, 1 - c)
    heavies = (heavy(1), heavy(-1))
    lights = (light(1), light(-1), light(2))
    aheads = {d: along(d) for d in (1, -1, 2, -2)}
    h_peers = [(a, x, y, lax.rem(h + d, nh), c) for d in range(1, nh)]
    peers = [partner, *heavies, *lights, light(-2), *aheads.values(), *h_peers]

    def rel(v, d):
        return lax.rem(v + d, 4)

    def yrel(d):
        return lax.rem(y + d + ny, ny)

    def owner(cc, qq, yy, pp):
        return ((qq + cc * (pp - qq)) * 4 + (pp + cc * (qq - pp))) * ny + yy

    def remote(src, dst, s, r, to):
        return pltpu.make_async_remote_copy(
            src_ref=src, dst_ref=dst, send_sem=s, recv_sem=r, device_id=to, device_id_type=MESH
        )

    mine = (q * ny + y) * 4 + p
    load_w = pltpu.make_async_copy(
        weight.at[:, pl.ds(pl.multiple_of(c * hw, hw), hw)], gow.at[c, mine], loc.at[0]
    )
    load_order = pltpu.make_async_copy(order_in, order, loc.at[1])
    loads = [
        pltpu.make_async_copy(
            cot.at[m, :, pl.ds(k * hw, hw)], cv.at[k, pl.ds(m * tok, tok)], loc.at[2 + 2 * m + k]
        )
        for m in range(micro)
        for k in range(2)
    ]
    loads.append(load_order)
    wide = width // 2
    wides = [
        [
            pltpu.make_async_copy(
                normed.at[m, :, pl.ds(k * wide, wide)],
                nv.at[pl.ds(m * tok, tok), pl.ds(k * wide, wide)],
                loc.at[2 + (2 + k) * micro + m],
            )
            for m in range(micro)
        ]
        for k in range(2)
    ]
    load_m = [
        pltpu.make_async_copy(main.at[:, pl.ds(k * hw, hw)], mv.at[k], loc.at[2 + 4 * micro + k]) for k in range(2)
    ]
    load_w.start()
    for copy in wides[0] + wides[1] + loads + load_m:
        copy.start()

    barrier = pltpu.get_barrier_semaphore()
    for peer in peers:
        pl.semaphore_signal(barrier, inc=1, device_id=peer, device_id_type=MESH)

    chunks = width // CHUNK
    sent = []

    def send(copy, group, size):
        copy.start()
        sent.append((group, size))
        return copy

    def turn(i, carry):
        at = pl.multiple_of(i * CHUNK, CHUNK)
        block = nv[:, pl.ds(at, CHUNK)].T
        turned[pl.ds(i * blocks_in_chunk, blocks_in_chunk)] = block.reshape(blocks_in_chunk, rows, micro * tok)
        return carry

    def gradient(cc, qq, u):
        which = [owner(cc, qq, yrel(d), pp) for d in UNITS[u] for pp in range(4)]
        block = jnp.concatenate([turned[order[0, f]] for f in which], axis=0)
        return jnp.dot(block, cv[cc], preferred_element_type=F32).reshape(8, rows, hw)

    def unit(qq, u):
        return pl.ds((qq * 4 + u) * 8, 8)

    def prepare():
        for k in range(2):
            for copy in wides[k]:
                copy.wait()
            lax.fori_loop(k * chunks // 2, (k + 1) * chunks // 2, turn, 0, unroll=2)
        for copy in loads:
            copy.wait()

    def partners(dq, u):
        qq = rel(p, dq)
        snd[unit(qq, u)] = gradient(1 - c, qq, u).astype(BF16)

    far = jnp.minimum(y, ny - y) // max(ny // 2 - 1, 1) * (h // max(nh - 1, 1))
    late = far > 0
    early = far == 0

    @pl.when(early)
    def _():
        prepare()
        for dq in (2, 1, 3, 0):
            for u in range(4):
                partners(dq, u)

    load_w.wait()
    pl.semaphore_wait(barrier, len(peers))
    own = gow.at[c, mine]
    ag_p = [send(remote(own, own, out.at[0], apr.at[k], lights[k]), 0, 1) for k in range(3)]

    pl.when(late)(prepare)

    rs_d = {}

    def give(dq):
        @pl.when(late)
        def _():
            for u in range(4):
                partners(dq, u)

        for u in range(4):
            ref = unit(rel(p, dq), u)
            rs_d[dq, u] = send(
                remote(snd.at[ref], rcv.at[ref], out.at[1], rdr.at[dq * 4 + u], partner), 1, 8
            )

    def summed(dq, u, extra=()):
        qq = rel(q, dq)
        v = gradient(c, qq, u) + rcv[unit(qq, u)].astype(F32)
        for ref in extra:
            v += ref[...].astype(F32)
        return v

    def to_sq(dq, u, extra=()):
        ref = unit(rel(q, dq), u)
        sq[ref] = summed(dq, u, extra).astype(BF16)
        return sq.at[ref]

    two_away = {PLUS: (0, 2), MINUS: (1, 3)}

    give(2)
    give(1)

    rs_t = {}
    for k in range(2):
        for way in (PLUS, MINUS):
            u = two_away[way][k]
            rs_d[2, u].wait_recv()
            rs_t[way, k] = send(
                remote(to_sq(2, u), tq.at[way, k], out.at[2], rqr.at[way, 4 + k], heavies[way]), 2, 8
            )

    give(3)

    for copy in ag_p:
        copy.wait_recv()

    def piece(dq, d):
        return gow.at[c, pl.ds((rel(q, dq) * ny + yrel(d)) * 4, 4)]

    def half_piece(d, j):
        return gow.at[c, pl.ds((q * ny + yrel(d)) * 4 + 2 * j, 2)]

    ag_y, ag_q = {}, {}

    def ag_along(k, d, ref, size):
        ag_y[k] = send(remote(ref, ref, out.at[3], ayr.at[k], aheads[d]), 3, size)

    def ag_heavy(way, dq, d, k):
        ref = piece(dq, d)
        ag_q[way, k] = send(remote(ref, ref, out.at[4], aqr.at[way, k], heavies[way]), 4, 4)

    def ag_across(dq, d):
        ref = piece(dq, d)
        send(remote(ref, ref, out.at[5], adr.at[0], partner), 5, 4)

    def ag_own(d):
        ag_heavy(PLUS, 0, d, d)
        ag_heavy(MINUS, 0, d, d)
        ag_across(0, d)

    ag_along(0, 2, piece(0, 0), 4)
    ag_along(1, -2, piece(0, 0), 4)
    ag_along(2, 1, piece(0, 0), 4)
    ag_along(3, -1, piece(0, 0), 4)

    give(0)

    rs_m = {}

    def rs_main(way, u, extra=()):
        dq = 1 if way == PLUS else 3
        rs_d[dq, u].wait_recv()
        rs_m[way, u] = send(
            remote(to_sq(dq, u, extra), mq.at[way, u], out.at[2], rqr.at[way, u], heavies[way]), 2, 8
        )

    rs_main(PLUS, 1)
    rs_main(MINUS, 0)
    rs_main(PLUS, 3)
    rs_main(MINUS, 2)

    lane = lax.broadcasted_iota(jnp.int32, (1, owners), 1)

    def invert(f, row):
        return jnp.where(lane == order[0, f], f, row)

    inv_row[...] = lax.fori_loop(0, owners, invert, jnp.zeros((1, owners), jnp.int32), unroll=8)
    load_inv = pltpu.make_async_copy(inv_row, inv, loc.at[0])
    load_inv.start()

    def carry(k):
        for way in (PLUS, MINUS):
            rs_t[way, k].wait_recv()
            rs_main(way, two_away[way][k], (tq.at[way, k],))

    carry(0)
    carry(1)
    ag_own(0)
    ag_y[0].wait_recv()
    ag_along(4, 1, piece(0, -2), 4)
    ag_along(6, 2, half_piece(-2, 0), 2)
    ag_y[1].wait_recv()
    ag_along(5, -1, piece(0, 2), 4)
    ag_along(7, -2, half_piece(2, 1), 2)
    ag_y[2].wait_recv()
    ag_own(7)
    ag_y[3].wait_recv()
    ag_own(1)
    ag_own(6)
    ag_own(2)

    def heavy_sum(u):
        rs_d[0, u].wait_recv()
        rs_m[PLUS, u].wait_recv()
        rs_m[MINUS, u].wait_recv()
        return summed(0, u, (mq.at[PLUS, u], mq.at[MINUS, u]))

    rs_y = {}

    def y_send(k, d, src, dst, size):
        rs_y[k] = send(remote(src, dst, out.at[6], ryr.at[k], aheads[d]), 6, size)

    sy[0] = heavy_sum(0).astype(BF16)
    y_send(0, 1, sy.at[0, pl.ds(0, 4)], ty.at[0], 4)
    y_send(2, 2, sy.at[0, pl.ds(4, 2)], hy.at[0], 2)
    y_send(3, -2, sy.at[0, pl.ds(6, 2)], hy.at[1], 2)
    v = heavy_sum(1)
    sy[1, pl.ds(0, 4)] = v[:4].astype(BF16)
    y_send(1, -1, sy.at[1, pl.ds(0, 4)], ty.at[1], 4)
    r2[1] = v[4:]
    v = heavy_sum(2)
    r2[2] = v[:4]
    sy[2, pl.ds(4, 4)] = v[4:].astype(BF16)
    y_send(4, 1, sy.at[2, pl.ds(4, 4)], my.at[0], 4)
    v = heavy_sum(3)
    sy[3, pl.ds(0, 4)] = v[:4].astype(BF16)
    y_send(5, -1, sy.at[3, pl.ds(0, 4)], my.at[1], 4)
    r2[0] = v[4:]

    forwards = {PLUS: (0, 1, 6, 3), MINUS: (7, 2, 5, 4)}

    def ag_arrived(d):
        for way in (PLUS, MINUS):
            ag_q[way, d].wait_recv()
            dq = 3 if way == PLUS else 1
            if d in forwards[way]:
                ag_heavy(way, dq, d, 8 + forwards[way].index(d))
            ag_across(dq, d)

    ag_arrived(0)
    ag_y[4].wait_recv()
    ag_own(5)
    ag_y[5].wait_recv()
    ag_own(3)
    ag_y[6].wait_recv()
    ag_y[7].wait_recv()
    ag_own(4)

    ag_arrived(7)
    ag_arrived(1)
    rs_y[0].wait_recv()
    rs_y[2].wait_recv()
    sy[2, pl.ds(0, 2)] = (r2[2, :2] + ty[0, :2].astype(F32) + hy[0].astype(F32)).astype(BF16)
    sy[2, pl.ds(2, 2)] = (r2[2, 2:] + ty[0, 2:].astype(F32)).astype(BF16)
    y_send(6, 2, sy.at[2, pl.ds(0, 4)], my.at[2], 4)
    rs_y[1].wait_recv()
    rs_y[3].wait_recv()
    sy[1, pl.ds(4, 2)] = (r2[1, :2] + ty[1, :2].astype(F32)).astype(BF16)
    sy[1, pl.ds(6, 2)] = (r2[1, 2:] + ty[1, 2:].astype(F32) + hy[1].astype(F32)).astype(BF16)
    y_send(7, -2, sy.at[1, pl.ds(4, 4)], my.at[3], 4)

    for d in (6, 2, 5, 3, 4):
        ag_arrived(d)
    for k in (4, 5, 6, 7):
        rs_y[k].wait_recv()
    v = r2[0]
    for k in range(4):
        v += my[k].astype(F32)
    r2[0] = v
    sy[3, pl.ds(4, 4)] = v.astype(BF16)
    rs_p = [
        send(remote(sy.at[3, 4 + rel(p, d)], pb.at[k], out.at[7], rpr.at[k], lights[k]), 7, 1)
        for k, d in enumerate((1, 3, 2))
    ]

    for k in range(4):
        for way in (PLUS, MINUS):
            ag_q[way, 8 + k].wait_recv()
            ag_across(2, forwards[way][k])

    for copy in rs_p:
        copy.wait_recv()
    value = r2[0, p]
    for k in range(3):
        value += pb[k].astype(F32)
    rounded = value.astype(BF16)
    sh[...] = rounded
    hb[h] = rounded
    rs_h = [send(remote(sh, hb.at[h], out.at[8], rhr.at[0], h_peers[d]), 8, 1) for d in range(nh - 1)]

    load_inv.wait()
    remote(gow.at[c], gow.at[1 - c], out.at[0], adr.at[0], partner).wait_recv()

    kacc[...] = jnp.zeros_like(kacc)
    contract = (((1,), (1,)), ((), ()))

    def product(i, carry):
        at = pl.ds(pl.multiple_of(i * CHUNK, CHUNK), CHUNK)
        fs = [inv[0, i * blocks_in_chunk + b] for b in range(blocks_in_chunk)]
        parts = [(lax.div(f, 4 * ny), lax.rem(lax.div(f, ny), 4), lax.rem(f, ny)) for f in fs]
        w0 = jnp.concatenate([gow[0, (fz * ny + fy) * 4 + fx] for fz, fx, fy in parts], axis=0)
        w1 = jnp.concatenate([gow[1, (fx * ny + fy) * 4 + fz] for fz, fx, fy in parts], axis=0)
        n = nv[:, at]
        kacc[0] += jnp.dot(n, w0, preferred_element_type=F32)
        kacc[1] += jnp.dot(n, w1, preferred_element_type=F32)
        g = lax.dot_general(cv[0], w0, contract, preferred_element_type=F32)
        g += lax.dot_general(cv[1], w1, contract, preferred_element_type=F32)
        ig_out[:, at] = g.astype(BF16)
        return carry

    lax.fori_loop(0, chunks, product, 0)
    key_out[:, :hw] = kacc[0].astype(BF16)
    key_out[:, hw:] = kacc[1].astype(BF16)

    def total(ref, n):
        return ref.at[pl.ds(0, n)]

    if nh > 1:
        ref = total(hb, nh - 1)
        remote(ref, ref, out.at[0], rhr.at[0], partner).wait_recv()
    for copy in load_m:
        copy.wait()
    value = hb[0].astype(F32)
    for k in range(1, nh):
        value += hb[k].astype(F32)
    fb[c] = mv[c] + value * scale
    last = send(remote(fb.at[c], fb.at[c], out.at[9], fin.at[0], partner), 9, 1)
    last.wait_recv()
    gb_out[:, :hw] = fb[0]
    gb_out[:, hw:] = fb[1]
    sizes = {}
    for group, size in sent:
        sizes[group] = sizes.get(group, 0) + size
    for group, size in sizes.items():
        ref = total(fb if group == 9 else snd, size)
        remote(ref, ref, out.at[group], fin.at[0], partner).wait_send()


def store(ig, key, gb, ig_out, key_out, gb_out, sems):
    micro, tok, width = ig_out.shape
    copies = [pltpu.make_async_copy(gb, gb_out, sems.at[2 * micro])]
    for m in range(micro):
        copies.append(pltpu.make_async_copy(ig.at[pl.ds(m * tok, tok)], ig_out.at[m], sems.at[m]))
        copies.append(pltpu.make_async_copy(key.at[pl.ds(m * tok, tok)], key_out.at[m], sems.at[micro + m]))
    for copy in copies:
        copy.start()
    for copy in copies:
        copy.wait()


def body(ny, nh, normed, kv_cotangent, kv_weight, main_grad, owner_order):
    micro, tok, width = normed.shape
    rows, key_width = kv_weight.shape
    owners = 16 * ny
    hw = key_width // 2
    everyone = owners * nh * 2
    scale = 1.0 / math.sqrt(micro * tok * everyone)
    dma = pltpu.SemaphoreType.DMA
    anywhere = pl.BlockSpec(memory_space=pl.ANY)
    vmem = pl.BlockSpec(memory_space=pltpu.VMEM)
    block = (rows, hw)
    all_rows = micro * tok
    key, ig, gb = pl.pallas_call(
        functools.partial(kernel, ny, nh, scale),
        out_shape=(
            pltpu.VMEM((all_rows, key_width), BF16),
            pltpu.VMEM((all_rows, width), BF16),
            pltpu.VMEM((rows, key_width), F32),
        ),
        in_specs=[anywhere] * 5,
        out_specs=(vmem,) * 3,
        scratch_shapes=[
            pltpu.SMEM((1, owners), jnp.int32),
            pltpu.SMEM((1, owners), jnp.int32),
            pltpu.VMEM((1, owners), jnp.int32),
            pltpu.VMEM((all_rows, width), BF16),
            pltpu.VMEM((2, all_rows, hw), BF16),
            pltpu.VMEM((2, *block), F32),
            pltpu.VMEM((owners, rows, all_rows), BF16),
            pltpu.VMEM((2, owners, *block), BF16),
            pltpu.VMEM((2, all_rows, hw), F32),
            pltpu.VMEM((owners, *block), BF16),
            pltpu.VMEM((owners, *block), BF16),
            pltpu.VMEM((owners, *block), BF16),
            pltpu.VMEM((2, 2, 8, *block), BF16),
            pltpu.VMEM((2, 4, 8, *block), BF16),
            pltpu.VMEM((4, 8, *block), BF16),
            pltpu.VMEM((2, 4, *block), BF16),
            pltpu.VMEM((2, 2, *block), BF16),
            pltpu.VMEM((4, 4, *block), BF16),
            pltpu.VMEM((3, 4, *block), F32),
            pltpu.VMEM((3, *block), BF16),
            pltpu.VMEM(block, BF16),
            pltpu.VMEM((nh, *block), BF16),
            pltpu.VMEM((2, *block), F32),
            dma((4 * micro + 4,)),
            dma((10,)),
            dma((3,)),
            dma((8,)),
            dma((2, 12)),
            dma((1,)),
            dma((16,)),
            dma((2, 6)),
            dma((8,)),
            dma((3,)),
            dma((1,)),
            dma((1,)),
        ],
        compiler_params=pltpu.CompilerParams(
            collective_id=0, has_side_effects=True, vmem_limit_bytes=56 * 1024 * 1024
        ),
    )(owner_order.reshape(1, owners), normed, kv_cotangent, kv_weight, main_grad)
    ig, key, gb = pl.pallas_call(
        store,
        out_shape=(
            jax.ShapeDtypeStruct((micro, tok, width), BF16),
            jax.ShapeDtypeStruct((micro, tok, key_width), BF16),
            jax.ShapeDtypeStruct((rows, key_width), F32),
        ),
        in_specs=[anywhere] * 3,
        out_specs=(anywhere,) * 3,
        scratch_shapes=[dma((2 * micro + 1,))],
        compiler_params=pltpu.CompilerParams(vmem_limit_bytes=1024 * 1024),
    )(ig, key, gb)
    return key, ig, gb


def solution(mesh):
    owners = mesh.shape["fsdp"]
    ny, nh = owners // 16, mesh.shape["dp"] // 2
    split = Mesh(mesh.devices.reshape(4, 4, ny, nh, 2), NAMES)
    tokens, fsdp = P(None, NAMES, None), P(NAMES[:3], None)
    return jax.shard_map(
        functools.partial(body, ny, nh),
        mesh=split,
        in_specs=(tokens, tokens, fsdp, fsdp, P()),
        out_specs=(tokens, tokens, fsdp),
        check_vma=False,
    )
```
